256 devices in a mesh: group: 2 (over z), blk: 128 (over y, x, core).
Axes of the slice: x: 8, y: 8, z: 2, core: 2. Of those that a mesh axis runs over, the one named last changes fastest.
The devices are a block of a 8x8x16 slice.
Arguments:
- tensors: bfloat16 [512, 256, 4, 256], P(('group', 'blk')), parts along dimension 0, may hold values from -6 to 6
- gate_terms: float32 [2, 16, 16], replicated, may hold values from -1.2 to 1.2
- right_proj: bfloat16 [256, 1024, 256], P('blk')
- left_proj: bfloat16 [256, 256, 1024], P('blk'), may hold values from -0.1875 to 0.1875
Outputs:
- evolved: bfloat16 [512, 256, 4, 256], P(('group', 'blk')), parts along dimension 0
- records: float32 [8, 2], P('group'), parts along dimension 0
The draws below stay inside these ranges and needn't reach their ends.
There are 2 independent parts, one for each index of `group`. The reference program is written for one: setup_inputs(seed, part) draws one part's arguments, and reference() takes and returns one part's arrays. A program takes and returns all parts, laid end to end along the dimension named above; an argument that names none is the same for every part. Nothing has to cross between parts.
All inputs are finite; a program needn't handle non-finite values.
Results may differ from the reference program's by a relative error of at most 0.024.
Values may be sent and summed in bfloat16 or wider, within the bound.
No kernel may reach another device: no remote copies, remote signals or barrier semaphores. Data moves between devices by JAX's collectives and lax.ppermute only.
A program may use at most 64 MiB of HBM per device.

```python
import math
import jax
import jax.numpy as jnp
from jax import lax

CHI = 256
D = 4
LAYERS = 4
SITES = 256
BONDS = 256


def draw_right_proj(key, part):
    base = jax.random.normal(key, (BONDS, D * CHI, CHI), jnp.float32) / math.sqrt(D * CHI)
    ramp = 1.0 + 0.05 * jnp.arange(BONDS, dtype=jnp.float32) / (BONDS - 1)
    return (base * ramp[:, None, None]).astype(jnp.bfloat16)


def block_levels(own_key, dims, shards, low, high):
    gain = 1.0
    for position, shards_of in shards:
        heights = jax.random.uniform(jax.random.fold_in(jax.random.fold_in(own_key, 6), position), (shards_of,), jnp.float32, low / len(shards), high / len(shards))
        gain = gain * jnp.repeat(jnp.exp(heights), dims[position] // shards_of).reshape((-1,) + (1,) * (len(dims) - 1 - position))
    return gain


def centred(own_key, extent, scale, limit, split=(), held_as=jnp.bfloat16):
    values = scale * jax.random.normal(own_key, extent, jnp.float32)
    if split:
        values = values * block_levels(own_key, extent, split, -0.22, 0.18)
    return jnp.clip(values, -limit, limit).astype(held_as)


def setup_inputs(seed: int = 0, part: int = 0) -> dict:
    key_of = jax.random.split(jax.random.key(seed), 5)
    part_keys = jax.random.split(jax.random.fold_in(key_of[4], part), 5)
    tensors = centred(part_keys[0], (SITES, CHI, D, CHI), 1.0, 6.0, ((0, 128),))
    gate_terms = centred(key_of[1], (2, D * D, D * D), 0.3, 1.2, (), jnp.float32)
    right_proj = draw_right_proj(jax.random.fold_in(key_of[4], 71), part)
    left_proj = centred(key_of[3], (BONDS, CHI, CHI * D), (CHI * D) ** -0.5, 0.1875, ((0, 128),))
    return {"tensors": tensors, "gate_terms": gate_terms, "right_proj": right_proj, "left_proj": left_proj}


def bond_update(left_site, right_site, gate_table, rproj_one, lproj_one):
    theta = jnp.dot(left_site.reshape(CHI * D, CHI), right_site.reshape(CHI, D * CHI), preferred_element_type=jnp.float32)
    theta_four = theta.reshape(CHI, D, D, CHI)
    gated = jnp.einsum('stuv,auvc->astc', gate_table, theta_four, precision=lax.Precision.HIGHEST)
    gated = gated.reshape(CHI * D, D * CHI).astype(jnp.bfloat16)
    fresh_left = jnp.dot(gated, rproj_one, preferred_element_type=jnp.float32)
    fresh_right = jnp.dot(lproj_one, gated, preferred_element_type=jnp.float32)
    return (fresh_left.reshape(CHI, D, CHI), fresh_right.reshape(CHI, D, CHI))

def reference(tensors, gate_terms, right_proj, left_proj):
    identity_matrix = jnp.eye(D * D, dtype=jnp.float32)
    entry_count = float(SITES * CHI * D * CHI)
    current = tensors
    rows_out = []
    for layer_index in range(LAYERS):
        parity = layer_index % 2
        gate_table = (identity_matrix + gate_terms[parity]).reshape(D, D, D, D)
        if parity == 0:
            lefts = current[0::2]
            rights = current[1::2]
        else:
            lefts = current[1::2]
            rights = jnp.roll(current, -1, axis=0)[1::2]

        def apply_pair(item):
            return bond_update(item[0], item[1], gate_table, item[2], item[3])
        fresh_left, fresh_right = lax.map(apply_pair, (lefts, rights, right_proj[parity::2], left_proj[parity::2]))
        updated = jnp.stack([fresh_left, fresh_right], axis=1).reshape(SITES, CHI, D, CHI)
        if parity == 1:
            updated = jnp.roll(updated, 1, axis=0)
        square_sum = jnp.sum(updated * updated)
        largest = jnp.max(jnp.abs(updated))
        root_mean = jnp.sqrt(square_sum / entry_count + 1e-06)
        rows_out.append(jnp.stack([jnp.log(root_mean), jnp.log(largest / root_mean)]))
        current = (updated / root_mean).astype(jnp.bfloat16)
    return (current, jnp.stack(rows_out))
```

```python
import functools

import jax
import jax.numpy as jnp
from jax import lax
from jax.experimental import pallas as pl
from jax.experimental.pallas import tpu as pltpu
from jax.sharding import PartitionSpec as P

CHI = 256
D = 4
ROWS = CHI * D
TILE = 16
LANES = 128
STEP = 16.0
LN2 = 0.6931471805599453
BF = jnp.bfloat16
F32 = jnp.float32


def iota(shape, dim):
    return lax.broadcasted_iota(jnp.int32, shape, dim)


def one_hot(mask):
    return jnp.where(mask, 1.0, 0.0).astype(BF)


def mm(a, b):
    return jnp.dot(a, b, preferred_element_type=F32)


def kron_gate(gate_terms):
    table = gate_terms + jnp.where(iota((TILE, TILE), 0) == iota((TILE, TILE), 1), 1.0, 0.0)
    left = one_hot((iota((256, TILE), 0) // TILE) == iota((256, TILE), 1))
    right = one_hot(iota((TILE, 256), 0) == (iota((TILE, 256), 1) // TILE))
    spread = mm(mm(left, table.astype(BF)).astype(BF), right)
    same = (iota((256, 256), 0) % TILE) == (iota((256, 256), 1) % TILE)
    return jnp.where(same, spread, 0.0).astype(BF)


def left_proj_order():
    row, col = iota((256, 256), 0), iota((256, 256), 1)
    return one_hot(((row % D) * 64 + row // D) == col)


def site_order():
    row, col = iota((256, 256), 0), iota((256, 256), 1)
    return one_hot(row == ((col % 8) * 32 + col // 8))


def site_order_back():
    row, col = iota((256, 256), 0), iota((256, 256), 1)
    return one_hot(((row % 8) * 32 + row // 8) == col)


def permute_left_proj(lproj_ref, out_ref):
    order = left_proj_order()
    for j in range(D):
        block = lproj_ref[:, j * 256 : (j + 1) * 256]
        out_ref[:, j * 256 : (j + 1) * 256] = mm(block, order).astype(BF)


def unpack_site(x_ref, site, out_ref):
    order = site_order()
    for i in range(4):
        pair = jnp.concatenate(
            [x_ref[site, (2 * i + k) * 256 : (2 * i + k + 1) * 256, :] for k in range(2)], axis=1
        )
        got = mm(order, pair).astype(BF)
        for k in range(2):
            for h in range(2):
                for u in range(D):
                    out_ref[
                        u * 256 + (2 * i + k) * 32 : u * 256 + (2 * i + k + 1) * 32,
                        h * LANES : (h + 1) * LANES,
                    ] = got[h * 128 + u * 32 : h * 128 + (u + 1) * 32, k * LANES : (k + 1) * LANES]


def theta_gate(left_ref, right_ref, kron, theta_ref, gated_ref):
    for v in range(D):
        block = mm(left_ref[...], right_ref[v * 256 : (v + 1) * 256, :]).astype(BF)
        for u in range(D):
            theta_ref[u * D + v] = block[u * 256 : (u + 1) * 256]
    for i in range(TILE):
        rhs = theta_ref[:, i * TILE : (i + 1) * TILE, :].reshape(256, 256)
        got = mm(kron, rhs).astype(BF)
        j, r = i // D, (i % D) * TILE
        for s in range(D):
            for t in range(D):
                row = j * 256 + s * 64 + r
                gated_ref[row : row + TILE, t * 256 : (t + 1) * 256] = got[
                    (s * D + t) * TILE : (s * D + t + 1) * TILE
                ]


def fold(acc, block):
    cube = block.reshape(32, 8, 256)
    square = jnp.sum(cube * cube, axis=0)
    largest = jnp.max(jnp.abs(cube), axis=0)
    if acc is None:
        return square, largest
    return acc[0] + square, jnp.maximum(acc[1], largest)


def fresh_left(gated_ref, rproj_ref, out_ref):
    acc = None
    for j in range(D):
        block = mm(gated_ref[j * 256 : (j + 1) * 256, :], rproj_ref[...])
        acc = fold(acc, block)
        block = block.astype(out_ref.dtype)
        for s in range(D):
            out_ref[s * 256 + j * 64 : s * 256 + (j + 1) * 64, :] = block[s * 64 : (s + 1) * 64]
    return acc


def fresh_right(gated_ref, lproj_ref, out_ref):
    acc = None
    for t in range(D):
        block = mm(lproj_ref[...], gated_ref[:, t * 256 : (t + 1) * 256])
        acc = fold(acc, block)
        out_ref[t * 256 : (t + 1) * 256, :] = block.astype(out_ref.dtype)
    return acc


def site_stats(acc):
    square = jnp.sum(jnp.sum(acc[0], axis=0, keepdims=True), axis=1, keepdims=True)
    largest = jnp.max(jnp.max(acc[1], axis=0, keepdims=True), axis=1, keepdims=True)
    square = jnp.broadcast_to(square, (8, LANES))
    largest = jnp.broadcast_to(largest, (8, LANES))
    log_square = jnp.log2(square)
    log_largest = jnp.log2(largest)
    steps = jnp.where(largest > 0.0, jnp.floor(log_largest / STEP + 0.5), 0.0)
    steps = jnp.clip(steps, -7.0, 7.0)
    return log_square, log_largest, steps


def stat_row(parts):
    lane = iota((8, LANES), 1)
    out = jnp.zeros((8, LANES), F32)
    for at, value in parts:
        out = jnp.where(lane == at, value, out)
    return out


def scale_rows(exponent, steps):
    down = jnp.exp2(steps * -STEP).astype(BF)
    total = (exponent + steps).astype(BF)
    both = jnp.concatenate([down.astype(F32), total.astype(F32)], axis=1)
    return jnp.concatenate([both, both], axis=0).astype(BF)


def finish_site(acc, exponent, lane, pay_ref):
    log_square, log_largest, steps = site_stats(acc)
    if pay_ref is not None:
        pay_ref[ROWS : ROWS + TILE, :] = scale_rows(exponent, steps)
    shift = exponent * STEP
    return [(lane, log_square + 2.0 * shift), (lane + 1, log_largest + shift)]


def scaled_copy(pay_ref, out_ref):
    scale = pay_ref[ROWS : ROWS + TILE, 0:LANES]
    scale = jnp.concatenate([scale, scale], axis=1)
    for i in range(ROWS // TILE):
        out_ref[i * TILE : (i + 1) * TILE, :] = pay_ref[i * TILE : (i + 1) * TILE, :] * scale


def exponent_of(pay_ref):
    return pay_ref[ROWS : ROWS + TILE, LANES : 2 * LANES][0:8].astype(F32)


def local_bond(parity, left, right, exponent, kron, theta, gated, rproj, lprojp, inter, intra, stat_in, stat, lane):
    theta_gate(left, right, kron, theta, gated)

    def both(left_out, right_out):
        acc_left = fresh_left(gated, rproj, left_out)
        acc_right = fresh_right(gated, lprojp, right_out)
        parts = finish_site(acc_left, exponent, lane, left_out)
        parts += finish_site(acc_right, exponent, lane + 2, right_out)
        row = stat_row(parts)
        stat[...] = row if stat_in is None else row + stat_in[...]

    @pl.when(parity == 0)
    def _():
        both(inter, intra)

    @pl.when(parity != 0)
    def _():
        both(intra, inter)


def prep_kernel(gates, lproj, lp_local, lp_cross, kron0, kron1):
    permute_left_proj(lproj.at[1], lp_cross)
    permute_left_proj(lproj.at[0], lp_local)
    kron0[...] = kron_gate(gates[0])
    kron1[...] = kron_gate(gates[1])


def first_kernel(parity, x, kron, rproj, lprojp, inter, intra, stat, left, right, theta, gated):
    unpack_site(x, 0, left)
    unpack_site(x, 1, right)
    exponent = jnp.zeros((8, LANES), F32)
    local_bond(
        parity[0], left, right, exponent, kron[...], theta, gated, rproj.at[0], lprojp, inter, intra, None, stat, 0
    )


def second_kernel(
    parity, inter_in, intra_in, kron, rproj, lprojp, stat_in, inter, intra, stat, left, right, theta, gated
):
    @pl.when(parity[0] == 0)
    def _():
        scaled_copy(inter_in, left)
        scaled_copy(intra_in, right)

    @pl.when(parity[0] != 0)
    def _():
        scaled_copy(intra_in, left)
        scaled_copy(inter_in, right)

    exponent = exponent_of(inter_in) + exponent_of(intra_in)
    local_bond(
        parity[0], left, right, exponent, kron[...], theta, gated, rproj.at[0], lprojp, inter, intra, stat_in, stat, 8
    )


def cross_kernel(
    flag, own, recv, kron, rproj, lprojp, stat_in, out, stat, *rest, lane, last
):
    left, right, theta, gated = rest[-4:]
    own_is_left = flag[0] != 0

    @pl.when(own_is_left)
    def _():
        scaled_copy(own, left)
        scaled_copy(recv, right)

    @pl.when(jnp.logical_not(own_is_left))
    def _():
        scaled_copy(recv, left)
        scaled_copy(own, right)

    theta_gate(left, right, kron[...], theta, gated)
    exponent = exponent_of(own) + exponent_of(recv)
    if last:
        rest[0][...] = exponent

    def done(acc):
        row = stat_in[0:8] + stat_row(finish_site(acc, exponent, lane, None if last else out))
        for i in range(stat.shape[0] // 8):
            stat[i * 8 : (i + 1) * 8, :] = jnp.broadcast_to(row[0:1], (8, LANES))

    @pl.when(own_is_left)
    def _():
        done(fresh_left(gated, rproj.at[1], out))

    @pl.when(jnp.logical_not(own_is_left))
    def _():
        done(fresh_right(gated, lprojp, out))


def final_kernel(parity, rows, inter, intra, inter_exp, intra_exp, out, records, left, obuf, sem, *, count):
    table = rows[...]
    peers = table.shape[0]
    largest = jnp.max(table, axis=0, keepdims=True)
    top = jnp.maximum(largest, -1e30)
    total = jnp.sum(jnp.exp2(table - top), axis=0, keepdims=True)

    def lane_value(x, at):
        return jnp.sum(jnp.where(iota((1, LANES), 1) == at, x, 0.0), axis=1, keepdims=True)

    log_scale = jnp.zeros((1, 1), F32)
    grid = jnp.zeros((8, LANES), F32)
    lane = iota((8, LANES), 1)
    row = iota((8, LANES), 0)
    for layer in range(4):
        at = 4 * layer
        tops = [lane_value(top, at + k) for k in (0, 2)]
        sums = [lane_value(total, at + k) for k in (0, 2)]
        peak = jnp.maximum(lane_value(largest, at + 1), lane_value(largest, at + 3))
        high = jnp.maximum(tops[0], tops[1])
        square = sums[0] * jnp.exp2(tops[0] - high) + sums[1] * jnp.exp2(tops[1] - high)
        log_square = jnp.log2(square) + high - 2.0 * log_scale
        mean = jnp.exp2(log_square) * (1.0 / count) + 1e-06
        log_root = 0.5 * jnp.log2(mean)
        first = log_root * LN2
        second = (peak - log_scale - log_root) * LN2
        grid = jnp.where((row == layer) & (lane == 0), first, grid)
        grid = jnp.where((row == layer) & (lane == 1), second, grid)
        if layer < 3:
            log_scale = 2.0 * (log_scale + log_root)
    records[...] = grid
    minus = jnp.broadcast_to(log_scale + log_root, (8, LANES))
    back = site_order_back()

    def write(site, src, exps):
        factor = jnp.exp2(exps[...] * STEP - minus)
        factor = jnp.concatenate([factor, factor], axis=1)
        for i in range(0, ROWS, 64):
            cube = src[i : i + 64, :].reshape(8, 8, 256) * factor[None]
            left[i : i + 64, :] = cube.reshape(64, 256).astype(BF)
        for i in range(4):
            cols = []
            for k in range(2):
                a = (2 * i + k) * 32
                cols.append(
                    jnp.concatenate(
                        [
                            left[u * 256 + a : u * 256 + a + 32, h * LANES : (h + 1) * LANES]
                            for h in range(2)
                            for u in range(D)
                        ],
                        axis=0,
                    )
                )
            got = mm(back, jnp.concatenate(cols, axis=1)).astype(BF)
            for k in range(2):
                obuf[site, (2 * i + k) * 256 : (2 * i + k + 1) * 256, :] = got[:, k * LANES : (k + 1) * LANES]

    @pl.when(parity[0] == 0)
    def _():
        write(0, inter, inter_exp)
        write(1, intra, intra_exp)

    @pl.when(parity[0] != 0)
    def _():
        write(0, intra, intra_exp)
        write(1, inter, inter_exp)

    copy = pltpu.make_async_copy(obuf, out, sem)
    copy.start()
    copy.wait()


VM = pl.BlockSpec(memory_space=pltpu.VMEM)
SM = pl.BlockSpec(memory_space=pltpu.SMEM)
HB = pl.BlockSpec(memory_space=pl.ANY)
PAY = pltpu.VMEM((ROWS + TILE, CHI), BF)
STAT = pltpu.VMEM((8, LANES), F32)
SITE = pltpu.VMEM((ROWS, CHI), F32)
KRON = pltpu.VMEM((256, 256), BF)
LPROJ = pltpu.VMEM((CHI, ROWS), BF)
WORK = [
    pltpu.VMEM((ROWS, CHI), BF),
    pltpu.VMEM((ROWS, CHI), BF),
    pltpu.VMEM((TILE, 256, 256), BF),
    pltpu.VMEM((ROWS, ROWS), BF),
]
GF = 1 << 30


def resident(x):
    return pltpu.with_memory_space_constraint(x, pltpu.MemorySpace.VMEM)


def call(kernel, outs, scratch, flops, scalars, arrays, out_specs=None):
    return pl.pallas_call(
        kernel,
        out_shape=outs,
        in_specs=[SM] * len(scalars) + [VM] * len(arrays),
        out_specs=out_specs or [VM] * len(outs),
        scratch_shapes=scratch,
        compiler_params=pltpu.CompilerParams(vmem_limit_bytes=16 << 20),
        cost_estimate=pl.CostEstimate(flops=flops, transcendentals=0, bytes_accessed=4 << 20),
    )(*scalars, *map(resident, arrays))


def local(tensors, gate_terms, right_proj, left_proj):
    slots = tensors.shape[0]
    peers = lax.axis_size("blk")
    count = float(peers * slots * CHI * D * CHI)
    parity = (lax.axis_index("blk") % 2).astype(jnp.int32).reshape(1)
    even = 1 - parity
    half = peers // 2
    intra_pairs = [(2 * k, 2 * k + 1) for k in range(half)] + [(2 * k + 1, 2 * k) for k in range(half)]
    inter_pairs = [(2 * k + 1, (2 * k + 2) % peers) for k in range(half)]
    inter_pairs += [((2 * k + 2) % peers, 2 * k + 1) for k in range(half)]

    x = tensors.reshape(slots, CHI, D, 2, LANES).transpose(0, 1, 3, 2, 4).reshape(slots, CHI * 8, LANES)

    lp_local, lp_cross, kron0, kron1 = call(
        prep_kernel, [LPROJ, LPROJ, KRON, KRON], [], GF // 4, [], [gate_terms, left_proj]
    )
    lp_inter = lax.ppermute(lp_cross, "blk", [(2 * k + 1, (2 * k + 2) % peers) for k in range(half)])
    lp_intra = lax.ppermute(lp_cross, "blk", [(2 * k, 2 * k + 1) for k in range(half)])

    inter, intra, stat = call(
        first_kernel, [PAY, PAY, STAT], WORK, 2 * GF, [parity], [x, kron0, right_proj, lp_local]
    )

    def swap(inter, intra):
        return lax.ppermute(inter, "blk", inter_pairs), lax.ppermute(intra, "blk", intra_pairs)

    def cross(flag, own, recv, lproj, stat, lane, last, rows=8):
        outs = [SITE if last else PAY, pltpu.VMEM((rows, LANES), F32)] + [STAT] * last
        return call(
            functools.partial(cross_kernel, lane=lane, last=last),
            outs,
            WORK,
            2 * GF,
            [flag],
            [own, recv, kron1, right_proj, lproj, stat],
        )

    inter_in, intra_in = swap(inter, intra)
    intra, stat = cross(even, intra, intra_in, lp_intra, stat, 4, False)
    inter, stat = cross(parity, inter, inter_in, lp_inter, stat, 6, False)

    inter, intra, stat = call(
        second_kernel, [PAY, PAY, STAT], WORK, 2 * GF, [parity], [inter, intra, kron0, right_proj, lp_local, stat]
    )

    inter_in, intra_in = swap(inter, intra)
    intra, stat, exp_intra = cross(even, intra, intra_in, lp_intra, stat, 12, True)
    inter, rows, exp_inter = cross(parity, inter, inter_in, lp_inter, stat, 14, True, peers)

    rows = lax.all_to_all(rows, "blk", 0, 0, tiled=True)

    out, records = call(
        functools.partial(final_kernel, count=count),
        [jax.ShapeDtypeStruct((slots, CHI * 8, LANES), BF), STAT],
        [
            pltpu.VMEM((ROWS, CHI), BF),
            pltpu.VMEM((slots, CHI * 8, LANES), BF),
            pltpu.SemaphoreType.DMA,
        ],
        1 << 26,
        [parity],
        [rows, inter, intra, exp_inter, exp_intra],
        [HB, VM],
    )
    evolved = out.reshape(slots, CHI, 2, D, LANES).transpose(0, 1, 3, 2, 4).reshape(slots, CHI, D, CHI)
    return evolved, records[:4, :2]


def solution(mesh):
    both = ("group", "blk")
    return jax.shard_map(
        local,
        mesh=mesh,
        in_specs=(P(both, None, None, None), P(), P("blk", None, None), P("blk", None, None)),
        out_specs=(P(both, None, None, None), P("group", None)),
        check_vma=False,
    )
```
